32 devices in a mesh: rep: 2 (over x), mp: 16 (over z, y, core).
Axes of the slice: x: 2, y: 2, z: 4, core: 2. Of those that a mesh axis runs over, the one named last changes fastest.
Arguments:
- tokens: bfloat16 [1280, 3072], P(('rep', 'mp')), may hold values from -6 to 6
- w_in: bfloat16 [2, 3072, 2, 12288], P('rep', None, None, 'mp'), may hold values from -0.109375 to 0.109375
- w_down: bfloat16 [2, 12288, 3072], P('rep', 'mp'), may hold values from -0.0546875 to 0.0546875
- norm_gain: float32 [3072], replicated, may hold values from 0.1 to 1.9
- final_gain: float32 [3072], replicated, may hold values from 0.1 to 1.9
- value_head: float32 [3072], replicated, may hold values from -0.6 to 0.6
- owner: int32 [16], P('mp'), may hold values from 0 to 1
- lengths: int32 [16], P('rep'), may hold values from 20 to 80, as said below
- offsets: int32 [16], P('rep'), may hold values from 0 to 620, as said below
Outputs:
- mixed: bfloat16 [1280, 3072], P(('rep', 'mp'))
- rewards: float32 [16], P('rep')
The draws below stay inside these ranges and needn't reach their ends.
Inputs may be any that keep to these rules, and one draw needn't show every extreme that they name: `lengths`: every rollout is at least a quarter of 80 long; in each group one rollout has exactly 80 tokens. `offsets`: rollout j of a group lies wholly within slots j * 80 to (j + 1) * 80 - 1 of its group; the other slots are padding.
All inputs are finite; a program needn't handle non-finite values.
Results may differ from the reference program's by a relative error of at most 0.0046.
Values may be sent and summed in bfloat16 or wider, within the bound.
No kernel may reach another device: no remote copies, remote signals or barrier semaphores. Data moves between devices by JAX's collectives and lax.ppermute only.
A program may use at most 128 MiB of HBM per device.

```python
import jax
import jax.numpy as jnp
from jax import lax

D = 3072
FF = 12288
SEQ_GRP = 8
GROUP_TOK = 640
TOKENS = 1280
MAX_LEN = 80
SEQS = 16
N_REP = 2
N_MP = 16


def packed_layout(base):
    drawn = jax.random.randint(base, (N_REP, SEQ_GRP), MAX_LEN // 4, MAX_LEN + 1)
    longest = jax.random.randint(jax.random.fold_in(base, 1), (N_REP,), 0, SEQ_GRP)
    column = jnp.arange(SEQ_GRP, dtype=jnp.int32)
    drawn = jnp.where(column[None, :] == longest[:, None], MAX_LEN, drawn).astype(jnp.int32)
    spare = (MAX_LEN - drawn + 1).astype(jnp.int32)
    shift_bits = jax.random.randint(jax.random.fold_in(base, 2), (N_REP, SEQ_GRP), 0, 1 << 20)
    shift = (shift_bits % spare).astype(jnp.int32)
    starts = (column[None, :] * MAX_LEN + shift).astype(jnp.int32)
    return (drawn.reshape(-1), starts.reshape(-1))


def draw_lengths(key, part):
    return packed_layout(jax.random.fold_in(key, 7))[0]


def draw_offsets(key, part):
    return packed_layout(jax.random.fold_in(key, 7))[1]


def with_ends(array, key, smallest, top_value):
    place = [jax.random.randint(jax.random.fold_in(key, axis), (), 0, length) for axis, length in enumerate(array.shape)]
    main_axis = array.shape.index(max(array.shape))
    beside = place[:main_axis] + [(place[main_axis] + 1) % array.shape[main_axis]] + place[main_axis + 1:]
    return array.at[tuple(place)].set(smallest).at[tuple(beside)].set(top_value)


def block_scale(rng, shape, pieces, low, top_value):
    def one(position, parts):
        heights = jax.random.uniform(jax.random.fold_in(jax.random.fold_in(rng, 6), position), (parts,), jnp.float32, low / len(pieces), top_value / len(pieces))
        return jnp.repeat(jnp.exp(heights), shape[position] // parts).reshape((-1,) + (1,) * (len(shape) - position - 1))

    factor_of = one(*pieces[0])
    for cut in pieces[1:]:
        factor_of = factor_of * one(*cut)
    return factor_of


def bell_draw(key, shape, spread, bound, shards=(), held_as=jnp.bfloat16):
    loudness = block_scale(key, shape, shards, -0.22, 0.18) if shards else 1.0
    values = jax.random.normal(key, shape, jnp.float32) * spread * loudness
    return jnp.minimum(jnp.maximum(values, -bound), bound).astype(held_as)


def setup_inputs(seed: int = 0) -> dict:
    keys = jax.random.split(jax.random.key(seed), 10)
    tokens = bell_draw(keys[0], (TOKENS, D), 1.0, 6.0, ((0, 32),))
    w_in = bell_draw(keys[1], (N_REP, D, 2, FF), D ** -0.5, 0.109375, ((0, 2), (3, 16)))
    w_down = bell_draw(keys[2], (N_REP, FF, D), FF ** -0.5, 0.0546875, ((0, 2), (1, 16)))
    norm_gain = jnp.clip(1.0 + 0.18 * jax.random.normal(keys[3], (D,), jnp.float32), 0.1, 1.9)
    final_gain = jnp.clip(1.0 + 0.18 * jax.random.normal(keys[4], (D,), jnp.float32), 0.1, 1.9)
    value_head = bell_draw(keys[5], (D,), 0.1, 0.6, (), jnp.float32)
    owner = with_ends(jax.random.randint(keys[6], (N_MP,), 0, N_REP), jax.random.fold_in(keys[6], 1), 0, N_REP - 1).astype(jnp.int32)
    lengths = draw_lengths(jax.random.fold_in(keys[9], 71), 0)
    offsets = draw_offsets(jax.random.fold_in(keys[9], 71), 0)
    return dict(tokens=tokens, w_in=w_in, w_down=w_down, norm_gain=norm_gain, final_gain=final_gain, value_head=value_head, owner=owner, lengths=lengths, offsets=offsets)


def reference(tokens, w_in, w_down, norm_gain, final_gain, value_head, owner, lengths, offsets):
    shard_cols = FF // N_MP
    shard_ids = jnp.arange(N_MP, dtype=jnp.int32)
    inner_split = w_in.reshape(N_REP, D, 2, N_MP, shard_cols)
    inner_chosen = jnp.transpose(inner_split[owner, :, :, shard_ids, :], (1, 2, 0, 3)).reshape(D, 2, FF)
    gate_weight = inner_chosen[:, 0, :]
    up_weight = inner_chosen[:, 1, :]
    down_weight = w_down.reshape(N_REP, N_MP, shard_cols, D)[owner, shard_ids].reshape(FF, D)
    grouped = tokens.reshape(N_REP, GROUP_TOK, D)
    group_lengths = lengths.reshape(N_REP, SEQ_GRP)
    group_offsets = offsets.reshape(N_REP, SEQ_GRP)

    def one_group(packed):
        block, seq_lengths, seq_offsets = packed
        slots = jnp.arange(GROUP_TOK, dtype=jnp.int32)
        member = ((slots[:, None] >= seq_offsets[None, :]) & (slots[:, None] < seq_offsets[None, :] + seq_lengths[None, :])).astype(jnp.float32)
        live = lax.optimization_barrier(jnp.sum(member, axis=1))
        block_f = block.astype(jnp.float32)
        normed = (block_f * lax.rsqrt(lax.optimization_barrier(jnp.mean(block_f * block_f, axis=1, keepdims=True)) + 1e-06) * norm_gain).astype(jnp.bfloat16)
        gate_part = jnp.dot(normed, gate_weight, preferred_element_type=jnp.float32)
        up_part = jnp.dot(normed, up_weight, preferred_element_type=jnp.float32)
        hidden = (jax.nn.gelu(gate_part, approximate=True) * up_part * live[:, None]).astype(jnp.bfloat16)
        resid = block_f + jnp.dot(hidden, down_weight, preferred_element_type=jnp.float32)
        final = resid * lax.rsqrt(lax.optimization_barrier(jnp.mean(resid * resid, axis=1, keepdims=True)) + 1e-06) * final_gain
        values = jnp.dot(final, value_head, precision=lax.Precision.HIGHEST)
        totals = jnp.dot(values, member, precision=lax.Precision.HIGHEST)
        return (resid.astype(jnp.bfloat16), totals / seq_lengths.astype(jnp.float32))
    mixed, rewards = lax.map(one_group, (grouped, group_lengths, group_offsets))
    return (mixed.reshape(TOKENS, D), rewards.reshape(SEQS))
```

```python
import functools

import jax
import jax.numpy as jnp
from jax import lax
from jax.experimental import pallas as pl
from jax.experimental.pallas import tpu as pltpu
from jax.sharding import PartitionSpec as P

AXES = ("rep", "mp")


def spread(value, axis, source):
    kept = jnp.where(lax.axis_index(axis) == source, value, 0).astype(value.dtype)
    return lax.psum(kept, axis)


def membership(slots, lengths, offsets):
    inside = (slots[:, None] >= offsets[None, :]) & (
        slots[:, None] < offsets[None, :] + lengths[None, :]
    )
    return inside.astype(jnp.float32)


def rms_normed(rows_f, gain):
    return rows_f * lax.rsqrt(jnp.mean(rows_f * rows_f, axis=1, keepdims=True) + 1e-06) * gain


def window_kernel(count, tile, own_ref, *refs):
    parts = refs[:count]
    in_ref, down_ref = refs[count : count + 2]
    outs = refs[count + 2 : 2 * count + 2]
    rows_ref, hidden_ref = refs[2 * count + 2 :]
    hidden, width = down_ref.shape
    spans = []
    start = 0
    for part in parts:
        spans.append((start, start + part.shape[0]))
        start += part.shape[0]

    @pl.when(own_ref[0] != 0)
    def _():
        for part, (low, high) in zip(parts, spans):
            rows_ref[low:high, :] = part[...]

        @pl.loop(0, hidden // tile)
        def _(step):
            at = pl.multiple_of(step * tile, tile)
            rows = rows_ref[...]
            gate = jnp.dot(rows, in_ref[:, pl.ds(at, tile)], preferred_element_type=jnp.float32)
            up_at = pl.multiple_of(hidden + at, tile)
            up = jnp.dot(rows, in_ref[:, pl.ds(up_at, tile)], preferred_element_type=jnp.float32)
            hidden_ref[:, pl.ds(at, tile)] = (jax.nn.gelu(gate, approximate=True) * up).astype(
                hidden_ref.dtype
            )

        wide = 2 * tile

        @pl.loop(0, width // wide)
        def _(step):
            at = pl.multiple_of(step * wide, wide)
            sums = jnp.dot(
                hidden_ref[...], down_ref[:, pl.ds(at, wide)], preferred_element_type=jnp.float32
            )
            for out, (low, high) in zip(outs, spans):
                out[:, pl.ds(at, wide)] = sums[low:high, :].astype(out.dtype)

    @pl.when(own_ref[0] == 0)
    def _():
        for out in outs:
            out[...] = jnp.zeros_like(out)


def window(own, parts, inner, outer):
    count = len(parts)
    rows = sum(part.shape[0] for part in parts)
    hidden, width = outer.shape
    tile = 256 if hidden % 256 == 0 else 128
    vmem = pl.BlockSpec(memory_space=pltpu.VMEM)
    held = 2 * (5 * rows * width + rows * hidden)
    return pl.pallas_call(
        functools.partial(window_kernel, count, tile),
        out_shape=[jax.ShapeDtypeStruct(part.shape, part.dtype) for part in parts],
        in_specs=[pl.BlockSpec(memory_space=pltpu.SMEM)] + [vmem] * (count + 2),
        out_specs=[vmem] * count,
        scratch_shapes=[
            pltpu.VMEM((rows, width), jnp.bfloat16),
            pltpu.VMEM((rows, hidden), jnp.bfloat16),
        ],
        compiler_params=pltpu.CompilerParams(
            vmem_limit_bytes=held + 2 * 3 * hidden * width
        ),
        cost_estimate=pl.CostEstimate(
            flops=6 * rows * width * hidden,
            bytes_accessed=4 * rows * width,
            transcendentals=rows * hidden,
        ),
        name="window",
    )(own, *parts, inner, outer)


def added(*terms):
    total = terms[0].astype(jnp.float32)
    for term in terms[1:]:
        total = total + term.astype(jnp.float32)
    return total.astype(terms[0].dtype)


def finish(resid, final_gain, value_head):
    return jnp.dot(
        rms_normed(resid, final_gain), value_head, precision=lax.Precision.HIGHEST
    )


def tokens_travel(n_mp, tokens, w_in, w_down, norm_gain, final_gain, value_head, owner, lengths, offsets):
    size, width = tokens.shape
    hidden = w_in.shape[3]
    depth = n_mp // 4

    def permute(value, target):
        moves = []
        for rep in range(2):
            for mp in range(n_mp):
                to_rep, to_mp = target(rep, mp)
                moves.append((rep * n_mp + mp, to_rep * n_mp + to_mp))
        return lax.ppermute(value, AXES, moves)

    def to_core(value):
        return permute(value, lambda rep, mp: (rep, mp ^ 1))

    def to_plane(value):
        return permute(value, lambda rep, mp: (1 - rep, mp) if mp % 2 == 0 else (rep, mp ^ 2))

    def to_depth(value, step):
        return permute(value, lambda rep, mp: (rep, mp ^ (4 * step)))

    own = (owner == lax.axis_index("rep")).astype(jnp.int32)
    inner = w_in.reshape(width, 2 * hidden)
    outer = w_down.reshape(hidden, width)
    tokens_f = tokens.astype(jnp.float32)
    normed = rms_normed(tokens_f, norm_gain).astype(jnp.bfloat16)

    order = [0] + list(range(depth - 1, 0, -1))
    arrived = {0: normed}
    for step in order[1:]:
        arrived[step] = to_depth(normed, step)
    sums = {}
    for step in order:
        mine = arrived[step]
        chip = jnp.concatenate([mine, to_core(mine)], axis=0)
        near = to_plane(chip)
        other = to_core(near)
        far = to_plane(other[:size])
        last = to_core(far)
        p_chip, p_near, p_other, p_far, p_last = window(
            own, [chip, near, other, far, last], inner, outer
        )
        p_far = added(p_far, to_core(p_last))
        p_other = jnp.concatenate(
            [added(p_other[:size], to_plane(p_far)), p_other[size:]], axis=0
        )
        p_near = added(p_near, to_core(p_other))
        p_chip = added(p_chip, to_plane(p_near))
        back = added(p_chip[:size], to_core(p_chip[size:]))
        sums[step] = to_depth(back, step) if step else back

    delta = sums[0].astype(jnp.float32)
    for step in order[1:]:
        delta = delta + sums[step].astype(jnp.float32)
    own_slots = lax.axis_index("mp") * size + jnp.arange(size, dtype=jnp.int32)
    member = membership(own_slots, lengths, offsets)
    live = jnp.sum(member, axis=1)[:, None]
    resid = tokens_f + delta * live
    values = finish(resid, final_gain, value_head)
    totals = jnp.dot(values, member, precision=lax.Precision.HIGHEST)
    totals = totals + to_core(totals)
    others = [
        permute(totals, lambda rep, mp, step=step: (rep, mp ^ (2 * step)))
        for step in range(1, n_mp // 2)
    ]
    for other in others:
        totals = totals + other
    return resid.astype(jnp.bfloat16), totals / lengths.astype(jnp.float32)


def weights_travel(tokens, w_in, w_down, norm_gain, final_gain, value_head, owner, lengths, offsets):
    owner_index = owner[0]
    tok_rows, width = tokens.shape
    hidden_cols = w_in.shape[3]
    tokens_f = tokens.astype(jnp.float32)
    normed = rms_normed(tokens_f, norm_gain).astype(jnp.bfloat16)
    inner = spread(w_in, "rep", owner_index).reshape(width, 2 * hidden_cols)
    outer = spread(w_down, "rep", owner_index).reshape(hidden_cols, width)
    piece = lax.all_gather(normed, "mp", axis=0, tiled=True)
    slots = jnp.arange(piece.shape[0], dtype=jnp.int32)
    products = jnp.dot(piece, inner, preferred_element_type=jnp.float32)
    live = jnp.sum(membership(slots, lengths, offsets), axis=1)[:, None]
    hidden = (
        jax.nn.gelu(products[:, :hidden_cols], approximate=True) * products[:, hidden_cols:] * live
    ).astype(jnp.bfloat16)
    delta = lax.psum_scatter(
        jnp.dot(hidden, outer, preferred_element_type=jnp.float32),
        "mp",
        scatter_dimension=0,
        tiled=True,
    )
    resid = tokens_f + delta
    values = finish(resid, final_gain, value_head)
    own_slots = lax.axis_index("mp") * tok_rows + jnp.arange(tok_rows, dtype=jnp.int32)
    member = membership(own_slots, lengths, offsets)
    totals = lax.psum(jnp.dot(values, member, precision=lax.Precision.HIGHEST), "mp")
    return resid.astype(jnp.bfloat16), totals / lengths.astype(jnp.float32)


def solution(mesh):
    n_rep, n_mp = mesh.shape["rep"], mesh.shape["mp"]
    pair = n_rep == 2 and n_mp % 4 == 0 and n_mp & (n_mp - 1) == 0
    body = functools.partial(tokens_travel, n_mp) if pair else weights_travel
    in_specs = (
        P(AXES, None),
        P("rep", None, None, "mp"),
        P("rep", "mp", None),
        P(),
        P(),
        P(),
        P("mp"),
        P("rep"),
        P("rep"),
    )
    return jax.shard_map(
        body, mesh=mesh, in_specs=in_specs, out_specs=(P(AXES, None), P("rep")), check_vma=False
    )
```

```python
import functools

import jax
import jax.numpy as jnp
from jax import lax
from jax.experimental import pallas as pl
from jax.experimental.pallas import tpu as pltpu
from jax.sharding import PartitionSpec as P


AXES = ("rep", "mp")


def spread(value, axis, source):
    kept = jnp.where(lax.axis_index(axis) == source, value, 0).astype(value.dtype)
    return lax.psum(kept, axis)


def membership(slots, lengths, offsets):
    inside = (slots[:, None] >= offsets[None, :]) & (
        slots[:, None] < offsets[None, :] + lengths[None, :]
    )
    return inside.astype(jnp.float32)


def rms_normed(rows_f, gain):
    return rows_f * lax.rsqrt(jnp.mean(rows_f * rows_f, axis=1, keepdims=True) + 1e-06) * gain


def window_kernel(count, tile, owner_ref, *refs):
    owned = owner_ref[0] == lax.axis_index("rep")
    parts = refs[:count]
    in_ref, down_ref = refs[count : count + 2]
    outs = refs[count + 2 : 2 * count + 2]
    rows_ref, hidden_ref = refs[2 * count + 2 :]
    hidden, width = down_ref.shape
    spans = []
    start = 0
    for part in parts:
        spans.append((start, start + part.shape[0]))
        start += part.shape[0]

    @pl.when(owned)
    def _():
        for part, (low, high) in zip(parts, spans):
            rows_ref[low:high, :] = part[...]

        rows = rows_ref[...]
        for at in range(0, hidden, tile):
            gate = jnp.dot(rows, in_ref[:, at : at + tile], preferred_element_type=jnp.float32)
            up_at = hidden + at
            up = jnp.dot(
                rows, in_ref[:, up_at : up_at + tile], preferred_element_type=jnp.float32
            )
            hidden_ref[:, at : at + tile] = (jax.nn.gelu(gate, approximate=True) * up).astype(
                hidden_ref.dtype
            )
        wide = 2 * tile
        for at in range(0, width, wide):
            sums = jnp.dot(
                hidden_ref[...], down_ref[:, at : at + wide], preferred_element_type=jnp.float32
            )
            for out, (low, high) in zip(outs, spans):
                out[:, at : at + wide] = sums[low:high, :].astype(out.dtype)

    @pl.when(jnp.logical_not(owned))
    def _():
        for out in outs:
            out[...] = jnp.zeros_like(out)


def window(owner, parts, inner, outer):
    count = len(parts)
    rows = sum(part.shape[0] for part in parts)
    hidden, width = outer.shape
    tile = 256 if hidden % 256 == 0 else 128
    vmem = pl.BlockSpec(memory_space=pltpu.VMEM)
    return pl.pallas_call(
        functools.partial(window_kernel, count, tile),
        out_shape=[jax.ShapeDtypeStruct(part.shape, part.dtype) for part in parts],
        in_specs=[pl.BlockSpec(memory_space=pltpu.SMEM)] + [vmem] * (count + 2),
        out_specs=[vmem] * count,
        scratch_shapes=[
            pltpu.VMEM((rows, width), jnp.bfloat16),
            pltpu.VMEM((rows, hidden), jnp.bfloat16),
        ],
        compiler_params=pltpu.CompilerParams(
            vmem_limit_bytes=2 * (3 * rows * width + 2 * rows * hidden)
        ),
        cost_estimate=pl.CostEstimate(
            flops=6 * rows * width * hidden,
            bytes_accessed=4 * rows * width,
            transcendentals=rows * hidden,
        ),
        name="window",
    )(owner, *parts, inner, outer)


def finish(resid, final_gain, value_head):
    return jnp.dot(
        rms_normed(resid, final_gain), value_head, precision=lax.Precision.HIGHEST
    )


def add_f32(*terms):
    total = terms[0].astype(jnp.float32)
    for term in terms[1:]:
        total = total + term.astype(jnp.float32)
    return total


def norm_kernel(tokens_ref, gain_ref, out_ref):
    width = tokens_ref.shape[1]
    rows = tokens_ref[...].astype(jnp.float32)
    scale = lax.rsqrt(jnp.sum(rows * rows, axis=1, keepdims=True) / width + 1e-06)
    out_ref[...] = (rows * scale * gain_ref[...]).astype(out_ref.dtype)


def pick_kernel(x_ref, y_ref, *refs):
    out_ref = refs[-1]
    even = lax.axis_index("mp") % 2 == 0

    @pl.when(even)
    def _():
        out_ref[...] = y_ref[...]

    @pl.when(jnp.logical_not(even))
    def _():
        out_ref[...] = x_ref[...]


def stack_kernel(mine_ref, x_ref, y_ref, far_ref, out_ref):
    size = mine_ref.shape[0]
    for place, ref in enumerate((mine_ref, x_ref, y_ref, far_ref)):
        out_ref[place * size : (place + 1) * size] = ref[...]


def far_kernel(part_ref, back_ref, out_ref):
    low = 3 * out_ref.shape[0]
    out_ref[...] = add_f32(part_ref[low:], back_ref[low:]).astype(out_ref.dtype)


def near_kernel(part_ref, back_ref, far_ref, x_ref, y_ref):
    size = far_ref.shape[0]
    even = lax.axis_index("mp") % 2 == 0
    x_at, y_at = slice(size, 2 * size), slice(2 * size, 3 * size)
    for out, at, takes in ((x_ref, x_at, jnp.logical_not(even)), (y_ref, y_at, even)):

        @pl.when(takes)
        def _():
            out[...] = add_f32(part_ref[at], back_ref[at], far_ref[...]).astype(out.dtype)

        @pl.when(jnp.logical_not(takes))
        def _():
            out[...] = add_f32(part_ref[at], back_ref[at]).astype(out.dtype)


def own_kernel(part_ref, back_ref, x_ref, y_ref, out_ref):
    size = x_ref.shape[0]
    out_ref[...] = add_f32(
        part_ref[:size], back_ref[:size], x_ref[...], y_ref[...]
    ).astype(out_ref.dtype)


def local(kernel, args, shapes):
    vmem = pl.BlockSpec(memory_space=pltpu.VMEM)
    outs = [jax.ShapeDtypeStruct(shape, args[0].dtype) for shape in shapes]
    cost = 4 * args[0].size
    result = pl.pallas_call(
        kernel,
        out_shape=outs,
        in_specs=[vmem] * len(args),
        out_specs=[vmem] * len(outs),
        compiler_params=pltpu.CompilerParams(vmem_limit_bytes=4 << 20),
        cost_estimate=pl.CostEstimate(flops=cost, bytes_accessed=2 * cost, transcendentals=0),
    )(*args)
    return result if len(outs) > 1 else result[0]


def finish_kernel(count, size, lengths_ref, offsets_ref, tokens_ref, *refs):
    sums = refs[:count]
    gain_ref, head_ref, mixed_ref, totals_ref = refs[count:]
    width = tokens_ref.shape[1]
    delta = add_f32(*(part[...] for part in sums))
    slots = lax.axis_index("mp") * size + lax.broadcasted_iota(jnp.int32, (size, 1), 0)
    member = [
        jnp.where(
            (slots >= offsets_ref[seq]) & (slots < offsets_ref[seq] + lengths_ref[seq]), 1.0, 0.0
        )
        for seq in range(lengths_ref.shape[0])
    ]
    live = member[0]
    for column in member[1:]:
        live = live + column
    resid = tokens_ref[...].astype(jnp.float32) + delta * live
    mixed_ref[...] = resid.astype(mixed_ref.dtype)
    scale = lax.rsqrt(jnp.sum(resid * resid, axis=1, keepdims=True) / width + 1e-06)
    final = resid * scale * gain_ref[...]
    values = jnp.sum(final * head_ref[...], axis=1, keepdims=True)
    for seq, column in enumerate(member):
        total = jnp.sum(values * column, axis=0, keepdims=True)
        totals_ref[seq : seq + 1, :] = jnp.broadcast_to(total, (1, totals_ref.shape[1]))


def finish_rows(tokens, sums, final_gain, value_head, lengths, offsets):
    size, _ = tokens.shape
    smem = pl.BlockSpec(memory_space=pltpu.SMEM)
    vmem = pl.BlockSpec(memory_space=pltpu.VMEM)
    return pl.pallas_call(
        functools.partial(finish_kernel, len(sums), size),
        out_shape=[
            jax.ShapeDtypeStruct(tokens.shape, tokens.dtype),
            jax.ShapeDtypeStruct((lengths.shape[0], 128), jnp.float32),
        ],
        in_specs=[smem] * 2 + [vmem] * (len(sums) + 3),
        out_specs=[vmem] * 2,
        compiler_params=pltpu.CompilerParams(vmem_limit_bytes=8 << 20),
        cost_estimate=pl.CostEstimate(
            flops=10 * tokens.size, bytes_accessed=14 * tokens.size, transcendentals=size
        ),
        name="finish",
    )(lengths, offsets, tokens, *sums, final_gain[None, :], value_head[None, :])


def ready_kernel(later_ref, out_ref):
    out_ref[...] = jnp.zeros_like(out_ref)


def ready(later):
    return pl.pallas_call(
        ready_kernel,
        out_shape=jax.ShapeDtypeStruct((8, 128), jnp.float32),
        in_specs=[pl.BlockSpec(memory_space=pltpu.HBM)],
        out_specs=pl.BlockSpec(memory_space=pltpu.VMEM),
        compiler_params=pltpu.CompilerParams(
            vmem_limit_bytes=50 << 20, has_side_effects=True
        ),
        name="ready",
    )(later)


def tokens_travel(n_mp, tokens, w_in, w_down, norm_gain, final_gain, value_head, owner, lengths, offsets):
    size, width = tokens.shape
    hidden = w_in.shape[3]
    depth = n_mp // 4

    def permute(value, target):
        moves = []
        for rep in range(2):
            for mp in range(n_mp):
                to_rep, to_mp = target(rep, mp)
                moves.append((rep * n_mp + mp, to_rep * n_mp + to_mp))
        return lax.ppermute(value, AXES, moves)

    def to_core(value):
        return permute(value, lambda rep, mp: (rep, mp ^ 1))

    def to_x(value):
        return permute(value, lambda rep, mp: (1 - rep, mp))

    def to_y(value):
        return permute(value, lambda rep, mp: (rep, mp ^ 2))

    def to_turn(value):
        return permute(value, lambda rep, mp: (rep, mp ^ 2) if mp % 2 else (1 - rep, mp))

    def to_depth(value, step):
        return permute(value, lambda rep, mp: (rep, mp ^ (4 * step)))

    inner = w_in.reshape(width, 2 * hidden)
    outer = w_down.reshape(hidden, width)
    ready(inner)
    normed = local(norm_kernel, (tokens, norm_gain[None, :]), [tokens.shape])

    order = [0] + list(range(depth - 1, 0, -1))
    arrived = {0: normed}
    for step in order[1:]:
        arrived[step] = to_depth(normed, step)
    sums = {}
    for step in order:
        mine = arrived[step]
        from_x = to_x(mine)
        from_y = to_y(mine)
        held = () if step else (outer,)
        turn = local(pick_kernel, (from_x, from_y, *held), [(size, width)])
        far = to_turn(turn)
        block = local(stack_kernel, (mine, from_x, from_y, far), [(4 * size, width)])
        other = to_core(block)
        part, part_other = window(owner, [block, other], inner, outer)
        back = to_core(part_other)
        far = local(far_kernel, (part, back), [(size, width)])
        far = to_turn(far)
        x_sum, y_sum = local(near_kernel, (part, back, far), [(size, width)] * 2)
        x_sum = to_x(x_sum)
        y_sum = to_y(y_sum)
        total = local(own_kernel, (part, back, x_sum, y_sum), [(size, width)])
        sums[step] = to_depth(total, step) if step else total

    mixed, totals = finish_rows(
        tokens, [sums[step] for step in order], final_gain, value_head, lengths, offsets
    )
    totals = totals[:, 0]
    shares = jnp.broadcast_to(totals[None, :], (n_mp, totals.shape[0]))
    totals = jnp.sum(lax.all_to_all(shares, "mp", 0, 0, tiled=True), axis=0)
    return mixed, totals / lengths.astype(jnp.float32)


def weights_travel(tokens, w_in, w_down, norm_gain, final_gain, value_head, owner, lengths, offsets):
    owner_index = owner[0]
    tok_rows, width = tokens.shape
    hidden_cols = w_in.shape[3]
    tokens_f = tokens.astype(jnp.float32)
    normed = rms_normed(tokens_f, norm_gain).astype(jnp.bfloat16)
    inner = spread(w_in, "rep", owner_index).reshape(width, 2 * hidden_cols)
    outer = spread(w_down, "rep", owner_index).reshape(hidden_cols, width)
    piece = lax.all_gather(normed, "mp", axis=0, tiled=True)
    slots = jnp.arange(piece.shape[0], dtype=jnp.int32)
    products = jnp.dot(piece, inner, preferred_element_type=jnp.float32)
    live = jnp.sum(membership(slots, lengths, offsets), axis=1)[:, None]
    hidden = (
        jax.nn.gelu(products[:, :hidden_cols], approximate=True) * products[:, hidden_cols:] * live
    ).astype(jnp.bfloat16)
    delta = lax.psum_scatter(
        jnp.dot(hidden, outer, preferred_element_type=jnp.float32),
        "mp",
        scatter_dimension=0,
        tiled=True,
    )
    resid = tokens_f + delta
    values = finish(resid, final_gain, value_head)
    own_slots = lax.axis_index("mp") * tok_rows + jnp.arange(tok_rows, dtype=jnp.int32)
    member = membership(own_slots, lengths, offsets)
    totals = lax.psum(jnp.dot(values, member, precision=lax.Precision.HIGHEST), "mp")
    return resid.astype(jnp.bfloat16), totals / lengths.astype(jnp.float32)


def solution(mesh):
    n_rep, n_mp = mesh.shape["rep"], mesh.shape["mp"]
    pair = n_rep == 2 and n_mp % 4 == 0 and n_mp & (n_mp - 1) == 0
    body = functools.partial(tokens_travel, n_mp) if pair else weights_travel

    in_specs = (
        P(AXES, None),
        P("rep", None, None, "mp"),
        P("rep", "mp", None),
        P(),
        P(),
        P(),
        P("mp"),
        P("rep"),
        P("rep"),
    )
    return jax.shard_map(
        body, mesh=mesh, in_specs=in_specs, out_specs=(P(AXES, None), P("rep")), check_vma=False
    )
```

```python
import functools

import jax
import jax.numpy as jnp
from jax import lax
from jax.experimental import pallas as pl
from jax.experimental.pallas import tpu as pltpu
from jax.sharding import PartitionSpec as P


AXES = ("rep", "mp")
RELAYS = 4
RELAY_GRANT = 53_000_000


def spread(value, axis, source):
    kept = jnp.where(lax.axis_index(axis) == source, value, 0).astype(value.dtype)
    return lax.psum(kept, axis)


def membership(slots, lengths, offsets):
    inside = (slots[:, None] >= offsets[None, :]) & (
        slots[:, None] < offsets[None, :] + lengths[None, :]
    )
    return inside.astype(jnp.float32)


def rms_normed(rows_f, gain):
    return rows_f * lax.rsqrt(jnp.mean(rows_f * rows_f, axis=1, keepdims=True) + 1e-06) * gain


def window_kernel(count, tile, owner_ref, *refs):
    owned = owner_ref[0] == lax.axis_index("rep")
    parts = refs[:count]
    outs = refs[-count - 2 : -2]
    rows_ref, hidden_ref = refs[-2:]
    in_refs, down_ref = refs[count : -count - 3], refs[-count - 3]
    hidden, width = down_ref.shape
    spans = []
    start = 0
    for part in parts:
        spans.append((start, start + part.shape[0]))
        start += part.shape[0]

    @pl.when(owned)
    def _():
        for part, (low, high) in zip(parts, spans):
            rows_ref[low:high, :] = part[...]

        def product(at):
            total = None
            for place, in_ref in enumerate(in_refs):
                depth = in_ref.shape[0]
                term = jnp.dot(
                    rows_ref[:, place * depth : (place + 1) * depth],
                    in_ref[:, at : at + tile],
                    preferred_element_type=jnp.float32,
                )
                total = term if total is None else total + term
            return total

        for at in range(0, hidden, tile):
            gate, up = product(at), product(hidden + at)
            hidden_ref[:, at : at + tile] = (jax.nn.gelu(gate, approximate=True) * up).astype(
                hidden_ref.dtype
            )
        wide = 2 * tile
        for at in range(0, width, wide):
            sums = jnp.dot(
                hidden_ref[...], down_ref[:, at : at + wide], preferred_element_type=jnp.float32
            )
            for out, (low, high) in zip(outs, spans):
                out[:, at : at + wide] = sums[low:high, :].astype(out.dtype)

    @pl.when(jnp.logical_not(owned))
    def _():
        for out in outs:
            out[...] = jnp.zeros_like(out)


def window(owner, parts, inner, outer):
    count = len(parts)
    rows = sum(part.shape[0] for part in parts)
    hidden, width = outer.shape
    tile = 256 if hidden % 256 == 0 else 128
    vmem = pl.BlockSpec(memory_space=pltpu.VMEM)
    return pl.pallas_call(
        functools.partial(window_kernel, count, tile),
        out_shape=[jax.ShapeDtypeStruct(part.shape, part.dtype) for part in parts],
        in_specs=[pl.BlockSpec(memory_space=pltpu.SMEM)] + [vmem] * (count + len(inner) + 1),
        out_specs=[vmem] * count,
        scratch_shapes=[
            pltpu.VMEM((rows, width), jnp.bfloat16),
            pltpu.VMEM((rows, hidden), jnp.bfloat16),
        ],
        compiler_params=pltpu.CompilerParams(
            vmem_limit_bytes=2 * (3 * rows * width + 2 * rows * hidden)
        ),
        cost_estimate=pl.CostEstimate(
            flops=6 * rows * width * hidden,
            bytes_accessed=4 * rows * width,
            transcendentals=rows * hidden,
        ),
        name="window",
    )(owner, *parts, *inner, outer)


def finish(resid, final_gain, value_head):
    return jnp.dot(
        rms_normed(resid, final_gain), value_head, precision=lax.Precision.HIGHEST
    )


def add_f32(*terms):
    total = terms[0].astype(jnp.float32)
    for term in terms[1:]:
        total = total + term.astype(jnp.float32)
    return total


def norm_kernel(tokens_ref, gain_ref, out_ref):
    width = tokens_ref.shape[1]
    rows = tokens_ref[...].astype(jnp.float32)
    scale = lax.rsqrt(jnp.sum(rows * rows, axis=1, keepdims=True) / width + 1e-06)
    out_ref[...] = (rows * scale * gain_ref[...]).astype(out_ref.dtype)


def pick_kernel(x_ref, y_ref, *refs):
    out_ref = refs[-1]
    even = lax.axis_index("mp") % 2 == 0

    @pl.when(even)
    def _():
        out_ref[...] = y_ref[...]

    @pl.when(jnp.logical_not(even))
    def _():
        out_ref[...] = x_ref[...]


def stack_kernel(mine_ref, x_ref, y_ref, far_ref, out_ref):
    size = mine_ref.shape[0]
    for place, ref in enumerate((mine_ref, x_ref, y_ref, far_ref)):
        out_ref[place * size : (place + 1) * size] = ref[...]


def far_kernel(part_ref, back_ref, out_ref):
    low = 3 * out_ref.shape[0]
    out_ref[...] = add_f32(part_ref[low:], back_ref[low:]).astype(out_ref.dtype)


def near_kernel(part_ref, back_ref, far_ref, x_ref, y_ref):
    size = far_ref.shape[0]
    even = lax.axis_index("mp") % 2 == 0
    x_at, y_at = slice(size, 2 * size), slice(2 * size, 3 * size)
    for out, at, takes in ((x_ref, x_at, jnp.logical_not(even)), (y_ref, y_at, even)):

        @pl.when(takes)
        def _():
            out[...] = add_f32(part_ref[at], back_ref[at], far_ref[...]).astype(out.dtype)

        @pl.when(jnp.logical_not(takes))
        def _():
            out[...] = add_f32(part_ref[at], back_ref[at]).astype(out.dtype)


def own_kernel(part_ref, back_ref, x_ref, y_ref, out_ref):
    size = x_ref.shape[0]
    out_ref[...] = add_f32(
        part_ref[:size], back_ref[:size], x_ref[...], y_ref[...]
    ).astype(out_ref.dtype)


def local(kernel, args, shapes):
    vmem = pl.BlockSpec(memory_space=pltpu.VMEM)
    outs = [jax.ShapeDtypeStruct(shape, args[0].dtype) for shape in shapes]
    cost = 4 * args[0].size
    result = pl.pallas_call(
        kernel,
        out_shape=outs,
        in_specs=[vmem] * len(args),
        out_specs=[vmem] * len(outs),
        compiler_params=pltpu.CompilerParams(vmem_limit_bytes=4 << 20),
        cost_estimate=pl.CostEstimate(flops=cost, bytes_accessed=2 * cost, transcendentals=0),
    )(*args)
    return result if len(outs) > 1 else result[0]


def finish_kernel(count, size, lengths_ref, offsets_ref, tokens_ref, *refs):
    sums = refs[:count]
    gain_ref, head_ref, mixed_ref, totals_ref = refs[count:]
    width = tokens_ref.shape[1]
    delta = add_f32(*(part[...] for part in sums))
    slots = lax.axis_index("mp") * size + lax.broadcasted_iota(jnp.int32, (size, 1), 0)
    member = [
        jnp.where(
            (slots >= offsets_ref[seq]) & (slots < offsets_ref[seq] + lengths_ref[seq]), 1.0, 0.0
        )
        for seq in range(lengths_ref.shape[0])
    ]
    live = member[0]
    for column in member[1:]:
        live = live + column
    resid = tokens_ref[...].astype(jnp.float32) + delta * live
    mixed_ref[...] = resid.astype(mixed_ref.dtype)
    scale = lax.rsqrt(jnp.sum(resid * resid, axis=1, keepdims=True) / width + 1e-06)
    final = resid * scale * gain_ref[...]
    values = jnp.sum(final * head_ref[...], axis=1, keepdims=True)
    for seq, column in enumerate(member):
        total = jnp.sum(values * column, axis=0, keepdims=True)
        totals_ref[seq : seq + 1, :] = jnp.broadcast_to(total, (1, totals_ref.shape[1]))


def finish_rows(tokens, sums, final_gain, value_head, lengths, offsets):
    size, _ = tokens.shape
    smem = pl.BlockSpec(memory_space=pltpu.SMEM)
    vmem = pl.BlockSpec(memory_space=pltpu.VMEM)
    return pl.pallas_call(
        functools.partial(finish_kernel, len(sums), size),
        out_shape=[
            jax.ShapeDtypeStruct(tokens.shape, tokens.dtype),
            jax.ShapeDtypeStruct((lengths.shape[0], 128), jnp.float32),
        ],
        in_specs=[smem] * 2 + [vmem] * (len(sums) + 3),
        out_specs=[vmem] * 2,
        compiler_params=pltpu.CompilerParams(vmem_limit_bytes=8 << 20),
        cost_estimate=pl.CostEstimate(
            flops=10 * tokens.size, bytes_accessed=14 * tokens.size, transcendentals=size
        ),
        name="finish",
    )(lengths, offsets, tokens, *sums, final_gain[None, :], value_head[None, :])


def relay_kernel(start, in_ref, out_ref, held_ref, sems):
    blocks, rows = held_ref.shape[0], held_ref.shape[1]
    loads = [
        pltpu.make_async_copy(
            in_ref.at[0, pl.ds(start + block * rows, rows)], held_ref.at[block], sems.at[block]
        )
        for block in range(blocks)
    ]
    for copy in loads:
        copy.start()
    for block, copy in enumerate(loads):
        copy.wait()
        out_ref[block * rows : (block + 1) * rows, :] = held_ref[block].reshape(
            rows, out_ref.shape[1]
        )


def relay(w_in, start, size, grant):
    _, _, sides, hidden = w_in.shape
    rows = 128 if size % 128 == 0 else size
    held = 2 * size * sides * hidden
    return pl.pallas_call(
        functools.partial(relay_kernel, start),
        out_shape=jax.ShapeDtypeStruct((size, sides * hidden), w_in.dtype),
        in_specs=[pl.BlockSpec(memory_space=pltpu.HBM)],
        out_specs=pl.BlockSpec(memory_space=pltpu.VMEM),
        scratch_shapes=[
            pltpu.VMEM((size // rows, rows, sides, hidden), w_in.dtype),
            pltpu.SemaphoreType.DMA((size // rows,)),
        ],
        compiler_params=pltpu.CompilerParams(vmem_limit_bytes=grant),
        cost_estimate=pl.CostEstimate(flops=held, bytes_accessed=2 * held, transcendentals=0),
        name="relay",
    )(w_in)


def tokens_travel(n_mp, tokens, w_in, w_down, norm_gain, final_gain, value_head, owner, lengths, offsets):
    size, width = tokens.shape
    hidden = w_in.shape[3]
    depth = n_mp // 4

    def permute(value, target):
        moves = []
        for rep in range(2):
            for mp in range(n_mp):
                to_rep, to_mp = target(rep, mp)
                moves.append((rep * n_mp + mp, to_rep * n_mp + to_mp))
        return lax.ppermute(value, AXES, moves)

    def to_core(value):
        return permute(value, lambda rep, mp: (rep, mp ^ 1))

    def to_x(value):
        return permute(value, lambda rep, mp: (1 - rep, mp))

    def to_y(value):
        return permute(value, lambda rep, mp: (rep, mp ^ 2))

    def to_turn(value):
        return permute(value, lambda rep, mp: (rep, mp ^ 2) if mp % 2 else (1 - rep, mp))

    def to_depth(value, step):
        return permute(value, lambda rep, mp: (rep, mp ^ (4 * step)))

    outer = w_down.reshape(hidden, width)
    depth_cut = width // RELAYS
    grant = RELAY_GRANT
    inner = []
    for piece in range(RELAYS):
        inner.append(relay(w_in, piece * depth_cut, depth_cut, grant))
        grant -= 4 * depth_cut * hidden
    normed = local(norm_kernel, (tokens, norm_gain[None, :]), [tokens.shape])

    order = [0] + list(range(depth - 1, 0, -1))
    arrived = {0: normed}
    for step in order[1:]:
        arrived[step] = to_depth(normed, step)
    sums = {}
    for step in order:
        mine = arrived[step]
        from_x = to_x(mine)
        from_y = to_y(mine)
        held = () if step else (outer,)
        turn = local(pick_kernel, (from_x, from_y, *held), [(size, width)])
        far = to_turn(turn)
        block = local(stack_kernel, (mine, from_x, from_y, far), [(4 * size, width)])
        other = to_core(block)
        part, part_other = window(owner, [block, other], inner, outer)
        back = to_core(part_other)
        far = local(far_kernel, (part, back), [(size, width)])
        far = to_turn(far)
        x_sum, y_sum = local(near_kernel, (part, back, far), [(size, width)] * 2)
        x_sum = to_x(x_sum)
        y_sum = to_y(y_sum)
        total = local(own_kernel, (part, back, x_sum, y_sum), [(size, width)])
        sums[step] = to_depth(total, step) if step else total

    mixed, totals = finish_rows(
        tokens, [sums[step] for step in order], final_gain, value_head, lengths, offsets
    )
    totals = totals[:, 0]
    shares = jnp.broadcast_to(totals[None, :], (n_mp, totals.shape[0]))
    totals = jnp.sum(lax.all_to_all(shares, "mp", 0, 0, tiled=True), axis=0)
    return mixed, totals / lengths.astype(jnp.float32)


def weights_travel(tokens, w_in, w_down, norm_gain, final_gain, value_head, owner, lengths, offsets):
    owner_index = owner[0]
    tok_rows, width = tokens.shape
    hidden_cols = w_in.shape[3]
    tokens_f = tokens.astype(jnp.float32)
    normed = rms_normed(tokens_f, norm_gain).astype(jnp.bfloat16)
    inner = spread(w_in, "rep", owner_index).reshape(width, 2 * hidden_cols)
    outer = spread(w_down, "rep", owner_index).reshape(hidden_cols, width)
    piece = lax.all_gather(normed, "mp", axis=0, tiled=True)
    slots = jnp.arange(piece.shape[0], dtype=jnp.int32)
    products = jnp.dot(piece, inner, preferred_element_type=jnp.float32)
    live = jnp.sum(membership(slots, lengths, offsets), axis=1)[:, None]
    hidden = (
        jax.nn.gelu(products[:, :hidden_cols], approximate=True) * products[:, hidden_cols:] * live
    ).astype(jnp.bfloat16)
    delta = lax.psum_scatter(
        jnp.dot(hidden, outer, preferred_element_type=jnp.float32),
        "mp",
        scatter_dimension=0,
        tiled=True,
    )
    resid = tokens_f + delta
    values = finish(resid, final_gain, value_head)
    own_slots = lax.axis_index("mp") * tok_rows + jnp.arange(tok_rows, dtype=jnp.int32)
    member = membership(own_slots, lengths, offsets)
    totals = lax.psum(jnp.dot(values, member, precision=lax.Precision.HIGHEST), "mp")
    return resid.astype(jnp.bfloat16), totals / lengths.astype(jnp.float32)


def solution(mesh):
    n_rep, n_mp = mesh.shape["rep"], mesh.shape["mp"]
    pair = n_rep == 2 and n_mp % 4 == 0 and n_mp & (n_mp - 1) == 0
    body = functools.partial(tokens_travel, n_mp) if pair else weights_travel

    in_specs = (
        P(AXES, None),
        P("rep", None, None, "mp"),
        P("rep", "mp", None),
        P(),
        P(),
        P(),
        P("mp"),
        P("rep"),
        P("rep"),
    )
    return jax.shard_map(
        body, mesh=mesh, in_specs=in_specs, out_specs=(P(AXES, None), P("rep")), check_vma=False
    )
```

```python
import functools

import jax
import jax.numpy as jnp
from jax import lax
from jax.experimental import pallas as pl
from jax.experimental.pallas import tpu as pltpu
from jax.sharding import PartitionSpec as P


AXES = ("rep", "mp")
RELAYS = 4
RELAY_GRANT = 53_000_000


def spread(value, axis, source):
    kept = jnp.where(lax.axis_index(axis) == source, value, 0).astype(value.dtype)
    return lax.psum(kept, axis)


def membership(slots, lengths, offsets):
    inside = (slots[:, None] >= offsets[None, :]) & (
        slots[:, None] < offsets[None, :] + lengths[None, :]
    )
    return inside.astype(jnp.float32)


def rms_normed(rows_f, gain):
    return rows_f * lax.rsqrt(jnp.mean(rows_f * rows_f, axis=1, keepdims=True) + 1e-06) * gain


def window_kernel(count, tile, owner_ref, *refs):
    owned = owner_ref[0] == lax.axis_index("rep")
    parts = refs[:count]
    outs = refs[-count - 2 : -2]
    rows_ref, hidden_ref = refs[-2:]
    in_refs, down_ref = refs[count : -count - 3], refs[-count - 3]
    hidden, width = down_ref.shape
    spans = []
    start = 0
    for part in parts:
        spans.append((start, start + part.shape[0]))
        start += part.shape[0]

    @pl.when(owned)
    def _():
        for part, (low, high) in zip(parts, spans):
            rows_ref[low:high, :] = part[...]

        def product(at):
            total = None
            for place, in_ref in enumerate(in_refs):
                depth = in_ref.shape[0]
                term = jnp.dot(
                    rows_ref[:, place * depth : (place + 1) * depth],
                    in_ref[:, at : at + tile],
                    preferred_element_type=jnp.float32,
                )
                total = term if total is None else total + term
            return total

        for at in range(0, hidden, tile):
            gate, up = product(at), product(hidden + at)
            hidden_ref[:, at : at + tile] = (jax.nn.gelu(gate, approximate=True) * up).astype(
                hidden_ref.dtype
            )
        wide = 2 * tile
        for at in range(0, width, wide):
            sums = jnp.dot(
                hidden_ref[...], down_ref[:, at : at + wide], preferred_element_type=jnp.float32
            )
            for out, (low, high) in zip(outs, spans):
                out[:, at : at + wide] = sums[low:high, :].astype(out.dtype)

    @pl.when(jnp.logical_not(owned))
    def _():
        for out in outs:
            out[...] = jnp.zeros_like(out)


def window(owner, parts, inner, outer):
    count = len(parts)
    rows = sum(part.shape[0] for part in parts)
    hidden, width = outer.shape
    tile = 256 if hidden % 256 == 0 else 128
    vmem = pl.BlockSpec(memory_space=pltpu.VMEM)
    return pl.pallas_call(
        functools.partial(window_kernel, count, tile),
        out_shape=[jax.ShapeDtypeStruct(part.shape, part.dtype) for part in parts],
        in_specs=[pl.BlockSpec(memory_space=pltpu.SMEM)] + [vmem] * (count + len(inner) + 1),
        out_specs=[vmem] * count,
        scratch_shapes=[
            pltpu.VMEM((rows, width), jnp.bfloat16),
            pltpu.VMEM((rows, hidden), jnp.bfloat16),
        ],
        compiler_params=pltpu.CompilerParams(
            vmem_limit_bytes=2 * (3 * rows * width + 2 * rows * hidden)
        ),
        cost_estimate=pl.CostEstimate(
            flops=6 * rows * width * hidden,
            bytes_accessed=4 * rows * width,
            transcendentals=rows * hidden,
        ),
        name="window",
    )(owner, *parts, *inner, outer)


def finish(resid, final_gain, value_head):
    return jnp.dot(
        rms_normed(resid, final_gain), value_head, precision=lax.Precision.HIGHEST
    )


def add_f32(*terms):
    total = terms[0].astype(jnp.float32)
    for term in terms[1:]:
        total = total + term.astype(jnp.float32)
    return total


def norm_kernel(tokens_ref, gain_ref, out_ref):
    width = tokens_ref.shape[1]
    rows = tokens_ref[...].astype(jnp.float32)
    scale = lax.rsqrt(jnp.sum(rows * rows, axis=1, keepdims=True) / width + 1e-06)
    out_ref[...] = (rows * scale * gain_ref[...]).astype(out_ref.dtype)


def pick_kernel(x_ref, y_ref, *refs):
    out_ref = refs[-1]
    even = lax.axis_index("mp") % 2 == 0

    @pl.when(even)
    def _():
        out_ref[...] = y_ref[...]

    @pl.when(jnp.logical_not(even))
    def _():
        out_ref[...] = x_ref[...]


def join_kernel(middle_ref, end_ref, out_ref):
    place = lax.axis_index("mp") // 4
    middle = (place == 1) | (place == 2)

    @pl.when(middle)
    def _():
        out_ref[...] = middle_ref[...]

    @pl.when(jnp.logical_not(middle))
    def _():
        out_ref[...] = end_ref[...]


def stack_kernel(mine_ref, x_ref, y_ref, far_ref, out_ref):
    size = mine_ref.shape[0]
    for place, ref in enumerate((mine_ref, x_ref, y_ref, far_ref)):
        out_ref[place * size : (place + 1) * size] = ref[...]


def far_kernel(part_ref, back_ref, out_ref):
    low = 3 * out_ref.shape[0]
    out_ref[...] = add_f32(part_ref[low:], back_ref[low:]).astype(out_ref.dtype)


def near_kernel(part_ref, back_ref, far_ref, x_ref, y_ref):
    size = far_ref.shape[0]
    even = lax.axis_index("mp") % 2 == 0
    x_at, y_at = slice(size, 2 * size), slice(2 * size, 3 * size)
    for out, at, takes in ((x_ref, x_at, jnp.logical_not(even)), (y_ref, y_at, even)):

        @pl.when(takes)
        def _():
            out[...] = add_f32(part_ref[at], back_ref[at], far_ref[...]).astype(out.dtype)

        @pl.when(jnp.logical_not(takes))
        def _():
            out[...] = add_f32(part_ref[at], back_ref[at]).astype(out.dtype)


def own_kernel(part_ref, back_ref, x_ref, y_ref, out_ref):
    size = x_ref.shape[0]
    out_ref[...] = add_f32(
        part_ref[:size], back_ref[:size], x_ref[...], y_ref[...]
    ).astype(out_ref.dtype)


def local(kernel, args, shapes):
    vmem = pl.BlockSpec(memory_space=pltpu.VMEM)
    outs = [jax.ShapeDtypeStruct(shape, args[0].dtype) for shape in shapes]
    cost = 4 * args[0].size
    result = pl.pallas_call(
        kernel,
        out_shape=outs,
        in_specs=[vmem] * len(args),
        out_specs=[vmem] * len(outs),
        compiler_params=pltpu.CompilerParams(vmem_limit_bytes=4 << 20),
        cost_estimate=pl.CostEstimate(flops=cost, bytes_accessed=2 * cost, transcendentals=0),
    )(*args)
    return result if len(outs) > 1 else result[0]


def finish_kernel(count, size, lengths_ref, offsets_ref, tokens_ref, *refs):
    sums = refs[:count]
    gain_ref, head_ref, mixed_ref, totals_ref = refs[count:]
    width = tokens_ref.shape[1]
    delta = add_f32(*(part[...] for part in sums))
    slots = lax.axis_index("mp") * size + lax.broadcasted_iota(jnp.int32, (size, 1), 0)
    member = [
        jnp.where(
            (slots >= offsets_ref[seq]) & (slots < offsets_ref[seq] + lengths_ref[seq]), 1.0, 0.0
        )
        for seq in range(lengths_ref.shape[0])
    ]
    live = member[0]
    for column in member[1:]:
        live = live + column
    resid = tokens_ref[...].astype(jnp.float32) + delta * live
    mixed_ref[...] = resid.astype(mixed_ref.dtype)
    scale = lax.rsqrt(jnp.sum(resid * resid, axis=1, keepdims=True) / width + 1e-06)
    final = resid * scale * gain_ref[...]
    values = jnp.sum(final * head_ref[...], axis=1, keepdims=True)
    for seq, column in enumerate(member):
        total = jnp.sum(values * column, axis=0, keepdims=True)
        totals_ref[seq : seq + 1, :] = jnp.broadcast_to(total, (1, totals_ref.shape[1]))


def finish_rows(tokens, sums, final_gain, value_head, lengths, offsets):
    size, _ = tokens.shape
    smem = pl.BlockSpec(memory_space=pltpu.SMEM)
    vmem = pl.BlockSpec(memory_space=pltpu.VMEM)
    return pl.pallas_call(
        functools.partial(finish_kernel, len(sums), size),
        out_shape=[
            jax.ShapeDtypeStruct(tokens.shape, tokens.dtype),
            jax.ShapeDtypeStruct((lengths.shape[0], 128), jnp.float32),
        ],
        in_specs=[smem] * 2 + [vmem] * (len(sums) + 3),
        out_specs=[vmem] * 2,
        compiler_params=pltpu.CompilerParams(vmem_limit_bytes=8 << 20),
        cost_estimate=pl.CostEstimate(
            flops=10 * tokens.size, bytes_accessed=14 * tokens.size, transcendentals=size
        ),
        name="finish",
    )(lengths, offsets, tokens, *sums, final_gain[None, :], value_head[None, :])


def relay_kernel(start, in_ref, out_ref, held_ref, sems):
    blocks, rows = held_ref.shape[0], held_ref.shape[1]
    loads = [
        pltpu.make_async_copy(
            in_ref.at[0, pl.ds(start + block * rows, rows)], held_ref.at[block], sems.at[block]
        )
        for block in range(blocks)
    ]
    for copy in loads:
        copy.start()
    for block, copy in enumerate(loads):
        copy.wait()
        out_ref[block * rows : (block + 1) * rows, :] = held_ref[block].reshape(
            rows, out_ref.shape[1]
        )


def relay(w_in, start, size, grant):
    _, _, sides, hidden = w_in.shape
    rows = 128 if size % 128 == 0 else size
    held = 2 * size * sides * hidden
    return pl.pallas_call(
        functools.partial(relay_kernel, start),
        out_shape=jax.ShapeDtypeStruct((size, sides * hidden), w_in.dtype),
        in_specs=[pl.BlockSpec(memory_space=pltpu.HBM)],
        out_specs=pl.BlockSpec(memory_space=pltpu.VMEM),
        scratch_shapes=[
            pltpu.VMEM((size // rows, rows, sides, hidden), w_in.dtype),
            pltpu.SemaphoreType.DMA((size // rows,)),
        ],
        compiler_params=pltpu.CompilerParams(vmem_limit_bytes=grant),
        cost_estimate=pl.CostEstimate(flops=held, bytes_accessed=2 * held, transcendentals=0),
        name="relay",
    )(w_in)


def tokens_travel(n_mp, tokens, w_in, w_down, norm_gain, final_gain, value_head, owner, lengths, offsets):
    size, width = tokens.shape
    hidden = w_in.shape[3]
    depth = n_mp // 4

    def permute(value, target):
        moves = []
        for rep in range(2):
            for mp in range(n_mp):
                to = target(rep, mp)
                if to is not None:
                    moves.append((rep * n_mp + mp, to[0] * n_mp + to[1]))
        return lax.ppermute(value, AXES, moves)

    def to_core(value):
        return permute(value, lambda rep, mp: (rep, mp ^ 1))

    def to_x(value):
        return permute(value, lambda rep, mp: (1 - rep, mp))

    def to_y(value):
        return permute(value, lambda rep, mp: (rep, mp ^ 2))

    def to_turn(value):
        return permute(value, lambda rep, mp: (rep, mp ^ 2) if mp % 2 else (1 - rep, mp))

    def to_depth(value, step):
        return permute(value, lambda rep, mp: (rep, mp ^ (4 * step)))

    outer = w_down.reshape(hidden, width)
    depth_cut = width // RELAYS
    grant = RELAY_GRANT
    inner = []
    for piece in range(RELAYS):
        inner.append(relay(w_in, piece * depth_cut, depth_cut, grant))
        grant -= 4 * depth_cut * hidden
    normed = local(norm_kernel, (tokens, norm_gain[None, :]), [tokens.shape])

    order = [0] + list(range(depth - 1, 0, -1))
    arrived = {0: normed}
    if depth == 4:
        arrived[1] = to_depth(normed, 1)

        def swap_middle(value):
            return permute(value, lambda rep, mp: (rep, mp ^ 12) if mp // 4 in (1, 2) else None)

        def to_ends(value):
            return permute(value, lambda rep, mp: (rep, mp ^ 4) if mp // 4 in (1, 2) else None)

        middle = swap_middle(normed)
        across = swap_middle(arrived[1])
        passed = to_ends(middle)
        arrived[2] = local(join_kernel, (across, passed), [(size, width)])
        passed = to_ends(across)
        arrived[3] = local(join_kernel, (middle, passed), [(size, width)])
    else:
        for step in order[1:]:
            arrived[step] = to_depth(normed, step)
    sums = {}
    for step in order:
        mine = arrived[step]
        from_x = to_x(mine)
        from_y = to_y(mine)
        held = () if step else (outer,)
        turn = local(pick_kernel, (from_x, from_y, *held), [(size, width)])
        far = to_turn(turn)
        block = local(stack_kernel, (mine, from_x, from_y, far), [(4 * size, width)])
        other = to_core(block)
        part, part_other = window(owner, [block, other], inner, outer)
        back = to_core(part_other)
        far = local(far_kernel, (part, back), [(size, width)])
        far = to_turn(far)
        x_sum, y_sum = local(near_kernel, (part, back, far), [(size, width)] * 2)
        x_sum = to_x(x_sum)
        y_sum = to_y(y_sum)
        total = local(own_kernel, (part, back, x_sum, y_sum), [(size, width)])
        sums[step] = to_depth(total, step) if step else total

    mixed, totals = finish_rows(
        tokens, [sums[step] for step in order], final_gain, value_head, lengths, offsets
    )
    totals = totals[:, 0]
    shares = jnp.broadcast_to(totals[None, :], (n_mp, totals.shape[0]))
    totals = jnp.sum(lax.all_to_all(shares, "mp", 0, 0, tiled=True), axis=0)
    return mixed, totals / lengths.astype(jnp.float32)


def weights_travel(tokens, w_in, w_down, norm_gain, final_gain, value_head, owner, lengths, offsets):
    owner_index = owner[0]
    tok_rows, width = tokens.shape
    hidden_cols = w_in.shape[3]
    tokens_f = tokens.astype(jnp.float32)
    normed = rms_normed(tokens_f, norm_gain).astype(jnp.bfloat16)
    inner = spread(w_in, "rep", owner_index).reshape(width, 2 * hidden_cols)
    outer = spread(w_down, "rep", owner_index).reshape(hidden_cols, width)
    piece = lax.all_gather(normed, "mp", axis=0, tiled=True)
    slots = jnp.arange(piece.shape[0], dtype=jnp.int32)
    products = jnp.dot(piece, inner, preferred_element_type=jnp.float32)
    live = jnp.sum(membership(slots, lengths, offsets), axis=1)[:, None]
    hidden = (
        jax.nn.gelu(products[:, :hidden_cols], approximate=True) * products[:, hidden_cols:] * live
    ).astype(jnp.bfloat16)
    delta = lax.psum_scatter(
        jnp.dot(hidden, outer, preferred_element_type=jnp.float32),
        "mp",
        scatter_dimension=0,
        tiled=True,
    )
    resid = tokens_f + delta
    values = finish(resid, final_gain, value_head)
    own_slots = lax.axis_index("mp") * tok_rows + jnp.arange(tok_rows, dtype=jnp.int32)
    member = membership(own_slots, lengths, offsets)
    totals = lax.psum(jnp.dot(values, member, precision=lax.Precision.HIGHEST), "mp")
    return resid.astype(jnp.bfloat16), totals / lengths.astype(jnp.float32)


def solution(mesh):
    n_rep, n_mp = mesh.shape["rep"], mesh.shape["mp"]
    pair = n_rep == 2 and n_mp % 4 == 0 and n_mp & (n_mp - 1) == 0
    body = functools.partial(tokens_travel, n_mp) if pair else weights_travel

    in_specs = (
        P(AXES, None),
        P("rep", None, None, "mp"),
        P("rep", "mp", None),
        P(),
        P(),
        P(),
        P("mp"),
        P("rep"),
        P("rep"),
    )
    return jax.shard_map(
        body, mesh=mesh, in_specs=in_specs, out_specs=(P(AXES, None), P("rep")), check_vma=False
    )
```

```python
import functools

import jax
import jax.numpy as jnp
from jax import lax
from jax.experimental import pallas as pl
from jax.experimental.pallas import tpu as pltpu
from jax.sharding import PartitionSpec as P


AXES = ("rep", "mp")
RELAYS = 4
RELAY_GRANT = 53_000_000


def spread(value, axis, source):
    kept = jnp.where(lax.axis_index(axis) == source, value, 0).astype(value.dtype)
    return lax.psum(kept, axis)


def membership(slots, lengths, offsets):
    inside = (slots[:, None] >= offsets[None, :]) & (
        slots[:, None] < offsets[None, :] + lengths[None, :]
    )
    return inside.astype(jnp.float32)


def rms_normed(rows_f, gain):
    return rows_f * lax.rsqrt(jnp.mean(rows_f * rows_f, axis=1, keepdims=True) + 1e-06) * gain


def window_kernel(count, tile, owner_ref, *refs):
    owned = owner_ref[0] == lax.axis_index("rep")
    parts = refs[:count]
    outs = refs[-count - 3 : -2]
    rows_ref, hidden_ref = refs[-2:]
    in_refs, down_ref = refs[count : -count - 4], refs[-count - 4]
    hidden, width = down_ref.shape
    spans = []
    start = 0
    for part in parts:
        spans.append((start, start + part.shape[0]))
        start += part.shape[0]
    out_spans = []
    start = 0
    for out in outs:
        out_spans.append((start, start + out.shape[0]))
        start += out.shape[0]

    @pl.when(owned)
    def _():
        for part, (low, high) in zip(parts, spans):
            rows_ref[low:high, :] = part[...]

        def product(at):
            total = None
            for place, in_ref in enumerate(in_refs):
                depth = in_ref.shape[0]
                term = jnp.dot(
                    rows_ref[:, place * depth : (place + 1) * depth],
                    in_ref[:, at : at + tile],
                    preferred_element_type=jnp.float32,
                )
                total = term if total is None else total + term
            return total

        for at in range(0, hidden, tile):
            gate, up = product(at), product(hidden + at)
            hidden_ref[:, at : at + tile] = (jax.nn.gelu(gate, approximate=True) * up).astype(
                hidden_ref.dtype
            )
        wide = 2 * tile
        for at in range(0, width, wide):
            sums = jnp.dot(
                hidden_ref[...], down_ref[:, at : at + wide], preferred_element_type=jnp.float32
            )
            for out, (low, high) in zip(outs, out_spans):
                out[:, at : at + wide] = sums[low:high, :].astype(out.dtype)

    @pl.when(jnp.logical_not(owned))
    def _():
        for out in outs:
            out[...] = jnp.zeros_like(out)


def window(owner, parts, inner, outer):
    count = len(parts)
    block = parts[-1].shape[0]
    out_rows = [part.shape[0] for part in parts[:-1]] + [block // 4 * 3, block // 4]
    rows = sum(part.shape[0] for part in parts)
    hidden, width = outer.shape
    tile = 256 if hidden % 256 == 0 else 128
    vmem = pl.BlockSpec(memory_space=pltpu.VMEM)
    return pl.pallas_call(
        functools.partial(window_kernel, count, tile),
        out_shape=[
            jax.ShapeDtypeStruct((size, width), parts[0].dtype) for size in out_rows
        ],
        in_specs=[pl.BlockSpec(memory_space=pltpu.SMEM)] + [vmem] * (count + len(inner) + 1),
        out_specs=[vmem] * len(out_rows),
        scratch_shapes=[
            pltpu.VMEM((rows, width), jnp.bfloat16),
            pltpu.VMEM((rows, hidden), jnp.bfloat16),
        ],
        compiler_params=pltpu.CompilerParams(
            vmem_limit_bytes=2 * (3 * rows * width + 2 * rows * hidden)
        ),
        cost_estimate=pl.CostEstimate(
            flops=6 * rows * width * hidden,
            bytes_accessed=4 * rows * width,
            transcendentals=rows * hidden,
        ),
        name="window",
    )(owner, *parts, *inner, outer)


def finish(resid, final_gain, value_head):
    return jnp.dot(
        rms_normed(resid, final_gain), value_head, precision=lax.Precision.HIGHEST
    )


def add_f32(*terms):
    total = terms[0].astype(jnp.float32)
    for term in terms[1:]:
        total = total + term.astype(jnp.float32)
    return total


def norm_kernel(tokens_ref, gain_ref, out_ref):
    width = tokens_ref.shape[1]
    rows = tokens_ref[...].astype(jnp.float32)
    scale = lax.rsqrt(jnp.sum(rows * rows, axis=1, keepdims=True) / width + 1e-06)
    out_ref[...] = (rows * scale * gain_ref[...]).astype(out_ref.dtype)


def pick_kernel(x_ref, y_ref, *refs):
    out_ref = refs[-1]
    even = lax.axis_index("mp") % 2 == 0

    @pl.when(even)
    def _():
        out_ref[...] = y_ref[...]

    @pl.when(jnp.logical_not(even))
    def _():
        out_ref[...] = x_ref[...]


def join_kernel(middle_ref, end_ref, out_ref):
    place = lax.axis_index("mp") // 4
    middle = (place == 1) | (place == 2)

    @pl.when(middle)
    def _():
        out_ref[...] = middle_ref[...]

    @pl.when(jnp.logical_not(middle))
    def _():
        out_ref[...] = end_ref[...]


def stack_kernel(mine_ref, x_ref, y_ref, far_ref, out_ref):
    size = mine_ref.shape[0]
    for place, ref in enumerate((mine_ref, x_ref, y_ref, far_ref)):
        out_ref[place * size : (place + 1) * size] = ref[...]


def far_kernel(part_ref, back_ref, out_ref):
    low = 3 * out_ref.shape[0]
    out_ref[...] = add_f32(part_ref[low:], back_ref[...]).astype(out_ref.dtype)


def near_kernel(part_ref, back_ref, far_ref, x_ref, y_ref):
    size = far_ref.shape[0]
    even = lax.axis_index("mp") % 2 == 0
    x_at, y_at = slice(size, 2 * size), slice(2 * size, 3 * size)
    for out, at, takes in ((x_ref, x_at, jnp.logical_not(even)), (y_ref, y_at, even)):

        @pl.when(takes)
        def _():
            out[...] = add_f32(part_ref[at], back_ref[at], far_ref[...]).astype(out.dtype)

        @pl.when(jnp.logical_not(takes))
        def _():
            out[...] = add_f32(part_ref[at], back_ref[at]).astype(out.dtype)


def own_kernel(part_ref, back_ref, x_ref, y_ref, out_ref):
    size = x_ref.shape[0]
    out_ref[...] = add_f32(
        part_ref[:size], back_ref[:size], x_ref[...], y_ref[...]
    ).astype(out_ref.dtype)


def local(kernel, args, shapes):
    vmem = pl.BlockSpec(memory_space=pltpu.VMEM)
    outs = [jax.ShapeDtypeStruct(shape, args[0].dtype) for shape in shapes]
    cost = 4 * args[0].size
    result = pl.pallas_call(
        kernel,
        out_shape=outs,
        in_specs=[vmem] * len(args),
        out_specs=[vmem] * len(outs),
        compiler_params=pltpu.CompilerParams(vmem_limit_bytes=4 << 20),
        cost_estimate=pl.CostEstimate(flops=cost, bytes_accessed=2 * cost, transcendentals=0),
    )(*args)
    return result if len(outs) > 1 else result[0]


def finish_kernel(count, size, lengths_ref, offsets_ref, tokens_ref, *refs):
    sums = refs[:count]
    gain_ref, head_ref, mixed_ref, totals_ref = refs[count:]
    width = tokens_ref.shape[1]
    delta = add_f32(*(part[...] for part in sums))
    slots = lax.axis_index("mp") * size + lax.broadcasted_iota(jnp.int32, (size, 1), 0)
    member = [
        jnp.where(
            (slots >= offsets_ref[seq]) & (slots < offsets_ref[seq] + lengths_ref[seq]), 1.0, 0.0
        )
        for seq in range(lengths_ref.shape[0])
    ]
    live = member[0]
    for column in member[1:]:
        live = live + column
    resid = tokens_ref[...].astype(jnp.float32) + delta * live
    mixed_ref[...] = resid.astype(mixed_ref.dtype)
    scale = lax.rsqrt(jnp.sum(resid * resid, axis=1, keepdims=True) / width + 1e-06)
    final = resid * scale * gain_ref[...]
    values = jnp.sum(final * head_ref[...], axis=1, keepdims=True)
    for seq, column in enumerate(member):
        total = jnp.sum(values * column, axis=0, keepdims=True)
        totals_ref[seq : seq + 1, :] = jnp.broadcast_to(total, (1, totals_ref.shape[1]))


def finish_rows(tokens, sums, final_gain, value_head, lengths, offsets):
    size, _ = tokens.shape
    smem = pl.BlockSpec(memory_space=pltpu.SMEM)
    vmem = pl.BlockSpec(memory_space=pltpu.VMEM)
    return pl.pallas_call(
        functools.partial(finish_kernel, len(sums), size),
        out_shape=[
            jax.ShapeDtypeStruct(tokens.shape, tokens.dtype),
            jax.ShapeDtypeStruct((lengths.shape[0], 128), jnp.float32),
        ],
        in_specs=[smem] * 2 + [vmem] * (len(sums) + 3),
        out_specs=[vmem] * 2,
        compiler_params=pltpu.CompilerParams(vmem_limit_bytes=8 << 20),
        cost_estimate=pl.CostEstimate(
            flops=10 * tokens.size, bytes_accessed=14 * tokens.size, transcendentals=size
        ),
        name="finish",
    )(lengths, offsets, tokens, *sums, final_gain[None, :], value_head[None, :])


def relay_kernel(start, in_ref, out_ref, held_ref, sems):
    blocks, rows = held_ref.shape[0], held_ref.shape[1]
    loads = [
        pltpu.make_async_copy(
            in_ref.at[0, pl.ds(start + block * rows, rows)], held_ref.at[block], sems.at[block]
        )
        for block in range(blocks)
    ]
    for copy in loads:
        copy.start()
    for block, copy in enumerate(loads):
        copy.wait()
        out_ref[block * rows : (block + 1) * rows, :] = held_ref[block].reshape(
            rows, out_ref.shape[1]
        )


def relay(w_in, start, size, grant):
    _, _, sides, hidden = w_in.shape
    rows = 128 if size % 128 == 0 else size
    held = 2 * size * sides * hidden
    return pl.pallas_call(
        functools.partial(relay_kernel, start),
        out_shape=jax.ShapeDtypeStruct((size, sides * hidden), w_in.dtype),
        in_specs=[pl.BlockSpec(memory_space=pltpu.HBM)],
        out_specs=pl.BlockSpec(memory_space=pltpu.VMEM),
        scratch_shapes=[
            pltpu.VMEM((size // rows, rows, sides, hidden), w_in.dtype),
            pltpu.SemaphoreType.DMA((size // rows,)),
        ],
        compiler_params=pltpu.CompilerParams(vmem_limit_bytes=grant),
        cost_estimate=pl.CostEstimate(flops=held, bytes_accessed=2 * held, transcendentals=0),
        name="relay",
    )(w_in)


def tokens_travel(n_mp, tokens, w_in, w_down, norm_gain, final_gain, value_head, owner, lengths, offsets):
    size, width = tokens.shape
    hidden = w_in.shape[3]
    depth = n_mp // 4

    def permute(value, target):
        moves = []
        for rep in range(2):
            for mp in range(n_mp):
                to = target(rep, mp)
                if to is not None:
                    moves.append((rep * n_mp + mp, to[0] * n_mp + to[1]))
        return lax.ppermute(value, AXES, moves)

    def to_core(value):
        return permute(value, lambda rep, mp: (rep, mp ^ 1))

    def to_x(value):
        return permute(value, lambda rep, mp: (1 - rep, mp))

    def to_y(value):
        return permute(value, lambda rep, mp: (rep, mp ^ 2))

    def to_turn(value):
        return permute(value, lambda rep, mp: (rep, mp ^ 2) if mp % 2 else (1 - rep, mp))

    def to_depth(value, step):
        return permute(value, lambda rep, mp: (rep, mp ^ (4 * step)))

    outer = w_down.reshape(hidden, width)
    depth_cut = width // RELAYS
    grant = RELAY_GRANT
    inner = []
    for piece in range(RELAYS):
        inner.append(relay(w_in, piece * depth_cut, depth_cut, grant))
        grant -= 4 * depth_cut * hidden
    normed = local(norm_kernel, (tokens, norm_gain[None, :]), [tokens.shape])

    order = [0] + list(range(depth - 1, 0, -1))
    arrived = {0: normed}
    if depth == 4:
        arrived[1] = to_depth(normed, 1)

        def swap_middle(value):
            return permute(value, lambda rep, mp: (rep, mp ^ 12) if mp // 4 in (1, 2) else None)

        def to_ends(value):
            return permute(value, lambda rep, mp: (rep, mp ^ 4) if mp // 4 in (1, 2) else None)

        middle = swap_middle(normed)
        across = swap_middle(arrived[1])
        passed = to_ends(middle)
        arrived[2] = local(join_kernel, (across, passed), [(size, width)])
        passed = to_ends(across)
        arrived[3] = local(join_kernel, (middle, passed), [(size, width)])
    else:
        for step in order[1:]:
            arrived[step] = to_depth(normed, step)
    sums = {}
    for step in order:
        mine = arrived[step]
        from_x = to_x(mine)
        from_y = to_y(mine)
        held = () if step else (outer,)
        turn = local(pick_kernel, (from_x, from_y, *held), [(size, width)])
        far = to_turn(turn)
        block = local(stack_kernel, (mine, from_x, from_y, far), [(4 * size, width)])
        other = to_core(block)
        part, part_near, part_far = window(owner, [block, other], inner, outer)
        back_far = to_core(part_far)
        back = to_core(part_near)
        far = local(far_kernel, (part, back_far), [(size, width)])
        far = to_turn(far)
        x_sum, y_sum = local(near_kernel, (part, back, far), [(size, width)] * 2)
        x_sum = to_x(x_sum)
        y_sum = to_y(y_sum)
        total = local(own_kernel, (part, back, x_sum, y_sum), [(size, width)])
        sums[step] = to_depth(total, step) if step else total

    mixed, totals = finish_rows(
        tokens, [sums[step] for step in order], final_gain, value_head, lengths, offsets
    )
    totals = totals[:, 0]
    shares = jnp.broadcast_to(totals[None, :], (n_mp, totals.shape[0]))
    totals = jnp.sum(lax.all_to_all(shares, "mp", 0, 0, tiled=True), axis=0)
    return mixed, totals / lengths.astype(jnp.float32)


def weights_travel(tokens, w_in, w_down, norm_gain, final_gain, value_head, owner, lengths, offsets):
    owner_index = owner[0]
    tok_rows, width = tokens.shape
    hidden_cols = w_in.shape[3]
    tokens_f = tokens.astype(jnp.float32)
    normed = rms_normed(tokens_f, norm_gain).astype(jnp.bfloat16)
    inner = spread(w_in, "rep", owner_index).reshape(width, 2 * hidden_cols)
    outer = spread(w_down, "rep", owner_index).reshape(hidden_cols, width)
    piece = lax.all_gather(normed, "mp", axis=0, tiled=True)
    slots = jnp.arange(piece.shape[0], dtype=jnp.int32)
    products = jnp.dot(piece, inner, preferred_element_type=jnp.float32)
    live = jnp.sum(membership(slots, lengths, offsets), axis=1)[:, None]
    hidden = (
        jax.nn.gelu(products[:, :hidden_cols], approximate=True) * products[:, hidden_cols:] * live
    ).astype(jnp.bfloat16)
    delta = lax.psum_scatter(
        jnp.dot(hidden, outer, preferred_element_type=jnp.float32),
        "mp",
        scatter_dimension=0,
        tiled=True,
    )
    resid = tokens_f + delta
    values = finish(resid, final_gain, value_head)
    own_slots = lax.axis_index("mp") * tok_rows + jnp.arange(tok_rows, dtype=jnp.int32)
    member = membership(own_slots, lengths, offsets)
    totals = lax.psum(jnp.dot(values, member, precision=lax.Precision.HIGHEST), "mp")
    return resid.astype(jnp.bfloat16), totals / lengths.astype(jnp.float32)


def solution(mesh):
    n_rep, n_mp = mesh.shape["rep"], mesh.shape["mp"]
    pair = n_rep == 2 and n_mp % 4 == 0 and n_mp & (n_mp - 1) == 0
    body = functools.partial(tokens_travel, n_mp) if pair else weights_travel

    in_specs = (
        P(AXES, None),
        P("rep", None, None, "mp"),
        P("rep", "mp", None),
        P(),
        P(),
        P(),
        P("mp"),
        P("rep"),
        P("rep"),
    )
    return jax.shard_map(
        body, mesh=mesh, in_specs=in_specs, out_specs=(P(AXES, None), P("rep")), check_vma=False
    )
```
